32 devices in a mesh: dp: 4 (over z), expert: 8 (over y, x, core).
Axes of the slice: x: 2, y: 2, z: 4, core: 2. Of those that a mesh axis runs over, the one named last changes fastest.
Arguments:
- tokens: bfloat16 [256, 192, 1024], P(None, ('dp', 'expert')), may hold values from -200 to 200
- grad_out: bfloat16 [256, 192, 1024], P(None, ('dp', 'expert')), may hold values from -6 to 6
- slot_out: bfloat16 [512, 192, 1024], P('expert', 'dp'), may hold values from -6 to 6
- slot_params: bfloat16 [512, 1024], P('expert'), may hold values from -2 to 2
Outputs:
- grad_tokens: bfloat16 [256, 192, 1024], P(None, ('dp', 'expert'))
- grad_slot_out: bfloat16 [512, 192, 1024], P('expert', 'dp')
- grad_params: float32 [512, 1024], P('expert', 'dp')
The draws below stay inside these ranges and needn't reach their ends.
All inputs are finite; a program needn't handle non-finite values.
Results may differ from the reference program's by a relative error of at most 0.018.
Values may be sent and summed in bfloat16 or wider, within the bound.
No kernel may reach another device: no remote copies, remote signals or barrier semaphores. Data moves between devices by JAX's collectives and lax.ppermute only.
A program may use at most 128 MiB of HBM per device.

```python
import math
import jax
import jax.numpy as jnp

D = 1024
SLOTS = 512
PATCHES = 256
IMAGES = 192


def slot_table(key):
    inner = jax.random.fold_in(key, 11)
    spread = 2.0 / math.sqrt(D)
    values = jnp.clip(jax.random.normal(inner, (SLOTS, D)) * spread, -6.0 * spread, 6.0 * spread)
    return values.astype(jnp.bfloat16).astype(jnp.float32)


def draw_slot_params(key, part):
    return slot_table(key).astype(jnp.bfloat16)


def draw_tokens(key, part):
    key_base = jax.random.fold_in(jax.random.fold_in(key, 23), 0)
    values = jnp.clip(jax.random.normal(key_base, (PATCHES, IMAGES, D)), -6.0, 6.0)
    return values.astype(jnp.bfloat16)


def block_levels(own_key, dims, pieces, smallest, largest):
    level, own = 1.0, jax.random.fold_in(own_key, 6)
    for axis_at, parts in pieces:
        steps = jnp.exp(jax.random.uniform(jax.random.fold_in(own, axis_at), (parts,), jnp.float32, smallest / len(pieces), largest / len(pieces)))
        level = level * jnp.repeat(steps, dims[axis_at] // parts).reshape([-1 if axis == axis_at else 1 for axis in range(len(dims))])
    return level


def gaussian(rng, dims, width, reach, cuts=(), kind=jnp.bfloat16):
    loudness = block_levels(rng, dims, cuts, -0.22, 0.18) if cuts else 1.0
    drawn = jax.random.normal(rng, dims, jnp.float32) * width * loudness
    return jnp.minimum(jnp.maximum(drawn, -reach), reach).astype(kind)


def setup_inputs(seed: int = 0) -> dict:
    key_of = jax.random.split(jax.random.key(seed), 5)
    return {
        "tokens": draw_tokens(jax.random.fold_in(key_of[4], 71), 0),
        "grad_out": gaussian(key_of[1], (PATCHES, IMAGES, D), 1.0, 6.0, ((1, 32),)),
        "slot_out": gaussian(key_of[2], (SLOTS, IMAGES, D), 1.0, 6.0, ((0, 8), (1, 4))),
        "slot_params": draw_slot_params(jax.random.fold_in(key_of[4], 71), 0),
    }


def reference(tokens, grad_out, slot_out, slot_params):
    tok_wide = tokens.astype(jnp.float32)
    grad_wide = grad_out.astype(jnp.float32)
    param_wide = slot_params.astype(jnp.float32)
    logits = jnp.einsum('tbd,sd->tbs', tok_wide, param_wide)
    combine = jax.nn.softmax(logits, axis=-1)
    combine_low = combine.astype(jnp.bfloat16)
    grad_slot = jnp.einsum('tbs,tbd->sbd', combine_low.astype(jnp.float32), grad_wide).astype(jnp.bfloat16)
    grad_comb = jnp.einsum('tbd,sbd->tbs', grad_wide, slot_out.astype(jnp.float32))
    rowdot = jnp.sum(combine * grad_comb, axis=-1, keepdims=True)
    grad_logits = (combine * (grad_comb - rowdot)).astype(jnp.bfloat16)
    logit_wide = grad_logits.astype(jnp.float32)
    grad_tok = jnp.einsum('tbs,sd->tbd', logit_wide, param_wide).astype(jnp.bfloat16)
    grad_params = jnp.einsum('tbs,tbd->sd', logit_wide, tok_wide)
    return grad_tok, grad_slot, grad_params
```

```python
import jax
import jax.numpy as jnp
from jax import lax
from jax.sharding import PartitionSpec as P


OUT_CHUNKS = 2
BACK_CHUNKS = 2


def partners(size, step):
    return [(i, i ^ step) for i in range(size)]


def trade(x, axis, step):
    return lax.ppermute(x, axis, partners(lax.axis_size(axis), step))


def gather_params(slot_params, owners, shards):
    shard = lax.axis_index("dp")
    own_slots, width = slot_params.shape
    cols = width // shards
    mine = lax.dynamic_slice_in_dim(slot_params, shard * cols, cols, axis=1)
    part = jnp.concatenate([mine] + [trade(mine, "expert", k) for k in range(1, owners)], axis=0)
    parts = jnp.stack([part] + [trade(part, "dp", j) for j in range(1, shards)])
    return jnp.concatenate(
        [lax.dynamic_index_in_dim(parts, j ^ shard, 0, keepdims=False) for j in range(shards)],
        axis=1,
    )


def fetch_outputs(slot_out, owners, me):
    own_slots, img_all, width = slot_out.shape
    size = own_slots // OUT_CHUNKS
    pieces = []
    for c in range(OUT_CHUNKS):
        chunk = slot_out[c * size : (c + 1) * size].transpose(1, 0, 2)
        chunk = chunk.reshape(owners, img_all // owners, size, width)
        for k in range(owners):
            block = lax.dynamic_index_in_dim(chunk, me ^ k, 0, keepdims=False)
            pieces.append(trade(block, "expert", k) if k else block)
    return jnp.concatenate(
        [pieces[c * owners + k] for k in range(owners) for c in range(OUT_CHUNKS)], axis=1
    )


def return_grads(grad_slot, owners, me):
    images, all_slots, width = grad_slot.shape
    own_slots = all_slots // owners
    size = own_slots // BACK_CHUNKS
    outs = []
    for c in range(BACK_CHUNKS):
        blocks = []
        for k in range(owners):
            at = k * own_slots + c * size
            block = grad_slot[:, at : at + size]
            blocks.append(trade(block, "expert", k) if k else block)
        buf = jnp.zeros((owners, images, size, width), grad_slot.dtype)
        for k in range(owners):
            buf = lax.dynamic_update_index_in_dim(buf, blocks[k], me ^ k, 0)
        outs.append(buf.reshape(owners * images, size, width).transpose(1, 0, 2))
    return jnp.concatenate(outs, axis=0)


def reduce_params(param_part, owners, shards):
    shard = lax.axis_index("dp")
    all_slots, width = param_part.shape
    cols, own_slots = width // shards, all_slots // owners
    low = param_part.astype(jnp.bfloat16)
    total = lax.dynamic_slice_in_dim(param_part, shard * cols, cols, axis=1)
    for j in range(1, shards):
        block = lax.dynamic_slice_in_dim(low, (shard ^ j) * cols, cols, axis=1)
        total = total + trade(block, "dp", j).astype(jnp.float32)
    low = total.astype(jnp.bfloat16)
    owned = total[:own_slots]
    for k in range(1, owners):
        block = low[k * own_slots : (k + 1) * own_slots]
        owned = owned + trade(block, "expert", k).astype(jnp.float32)
    return owned


def per_device(tokens, grad_out, slot_out, slot_params):
    owners, shards = lax.axis_size("expert"), lax.axis_size("dp")
    me = lax.axis_index("expert")
    all_params = gather_params(slot_params, owners, shards)
    slot_rows = fetch_outputs(slot_out, owners, me)
    logits = jnp.einsum("tbd,sd->tbs", tokens, all_params, preferred_element_type=jnp.float32)
    combine = jax.nn.softmax(logits, axis=-1)
    grad_slot = jnp.einsum(
        "tbs,tbd->bsd",
        combine.astype(jnp.bfloat16),
        grad_out,
        preferred_element_type=jnp.float32,
    ).astype(jnp.bfloat16)
    grad_slot_out = return_grads(grad_slot, owners, me)
    grad_comb = jnp.einsum("tbd,bsd->tbs", grad_out, slot_rows, preferred_element_type=jnp.float32)
    rowdot = jnp.sum(combine * grad_comb, axis=-1, keepdims=True)
    grad_logits = (combine * (grad_comb - rowdot)).astype(jnp.bfloat16)
    param_part = jnp.einsum("tbs,tbd->sd", grad_logits, tokens, preferred_element_type=jnp.float32)
    grad_params = reduce_params(param_part, owners, shards)
    grad_tok = jnp.einsum(
        "tbs,sd->tbd", grad_logits, all_params, preferred_element_type=jnp.float32
    ).astype(jnp.bfloat16)
    return (grad_tok, grad_slot_out, grad_params)


def solution(mesh):
    return jax.shard_map(
        per_device,
        mesh=mesh,
        in_specs=(
            P(None, ("dp", "expert"), None),
            P(None, ("dp", "expert"), None),
            P("expert", "dp", None),
            P("expert", None),
        ),
        out_specs=(P(None, ("dp", "expert"), None), P("expert", "dp", None), P("expert", "dp")),
        check_vma=False,
    )
```

```python
import jax
import jax.numpy as jnp
from jax import lax
from jax.experimental import pallas as pl
from jax.experimental.pallas import tpu as pltpu
from jax.sharding import PartitionSpec as P


UNITS = 4
OUT_UNITS = (1, 3)
BACK_UNITS = (3, 1)
LANES = 256


def partners(size, step):
    return [(i, i ^ step) for i in range(size)]


def trade(x, axis, step):
    return lax.ppermute(x, axis, partners(lax.axis_size(axis), step))


def gather_params(slot_params, owners, shards):
    shard = lax.axis_index("dp")
    _, width = slot_params.shape
    cols = width // shards
    mine = lax.dynamic_slice_in_dim(slot_params, shard * cols, cols, axis=1)
    blocks = [mine]
    for k in range(1, owners):
        blocks.append(trade(mine, "expert", k))
    part = jnp.concatenate(lax.optimization_barrier(blocks), axis=0)
    parts = [part]
    for j in range(1, shards):
        parts.append(trade(part, "dp", j))
    parts = jnp.stack(lax.optimization_barrier(parts))
    return jnp.concatenate(
        [lax.dynamic_index_in_dim(parts, j ^ shard, 0, keepdims=False) for j in range(shards)],
        axis=1,
    )


def split_kernel(me_ref, x_ref, *refs):
    outs, stage = refs[:-1], refs[-1]
    turned = x_ref[...].astype(jnp.float32).transpose(1, 0, 2).astype(x_ref.dtype)
    stage[...] = turned.reshape(stage.shape)
    for k, out in enumerate(outs):
        out[...] = stage[me_ref[0] ^ k]


def split_slots(slot_out, me, owners, first, units):
    own_slots, img_all, width = slot_out.shape
    unit, images = own_slots // UNITS, img_all // owners
    block = pl.BlockSpec((images, unit, LANES), lambda u, j, me: (0, u, j))
    return pl.pallas_call(
        split_kernel,
        out_shape=[jax.ShapeDtypeStruct((images, units * unit, width), slot_out.dtype)] * owners,
        grid_spec=pltpu.PrefetchScalarGridSpec(
            num_scalar_prefetch=1,
            grid=(units, width // LANES),
            in_specs=[pl.BlockSpec((unit, img_all, LANES), lambda u, j, me: (first + u, 0, j))],
            out_specs=[block] * owners,
            scratch_shapes=[pltpu.VMEM((owners, images, unit, LANES), slot_out.dtype)],
        ),
    )(me[None], slot_out)


def join_kernel(me_ref, *refs):
    stage, out = refs[-1], refs[-2]
    owners, images, unit, lanes = stage.shape
    for k in range(owners):
        stage[me_ref[0] ^ k] = refs[k][...]
    rows = stage[...].reshape(owners * images, unit, lanes)
    out[...] = rows.astype(jnp.float32).transpose(1, 0, 2).astype(out.dtype)


def join_slots(blocks, whole, me, own_slots, first, units):
    owners = len(blocks)
    images, _, width = blocks[0].shape
    unit = own_slots // UNITS
    block = pl.BlockSpec((images, unit, LANES), lambda u, j, me: (0, u, j))
    in_specs, extra, aliases = [block] * owners, [], {}
    if whole is not None:
        in_specs, extra, aliases = in_specs + [pl.BlockSpec(memory_space=pl.ANY)], [whole], {owners + 1: 0}
    return pl.pallas_call(
        join_kernel,
        out_shape=jax.ShapeDtypeStruct((own_slots, owners * images, width), blocks[0].dtype),
        grid_spec=pltpu.PrefetchScalarGridSpec(
            num_scalar_prefetch=1,
            grid=(units, width // LANES),
            in_specs=in_specs,
            out_specs=pl.BlockSpec(
                (unit, owners * images, LANES), lambda u, j, me: (first + u, 0, j)
            ),
            scratch_shapes=[pltpu.VMEM((owners, images, unit, LANES), blocks[0].dtype)],
        ),
        input_output_aliases=aliases,
    )(me[None], *blocks, *extra)


def fetch_outputs(slot_out, owners, me):
    parts, first = [], 0
    for units in OUT_UNITS:
        blocks = split_slots(slot_out, me, owners, first, units)
        got = [blocks[0]]
        for k in range(1, owners):
            got.append(trade(blocks[k], "expert", k))
        parts.append(got)
        first += units
    parts = lax.optimization_barrier(parts)
    return jnp.concatenate([part[k] for k in range(owners) for part in parts], axis=1)


def return_grads(grad_slot, owners, me):
    _, all_slots, _ = grad_slot.shape
    own_slots = all_slots // owners
    unit = own_slots // UNITS
    out, first = None, 0
    for units in BACK_UNITS:
        blocks = []
        for k in range(owners):
            at = k * own_slots + first * unit
            block = grad_slot[:, at : at + units * unit]
            blocks.append(trade(block, "expert", k) if k else block)
        out = join_slots(blocks, out, me, own_slots, first, units)
        first += units
    return out


def reduce_params(param_part, owners, shards):
    shard = lax.axis_index("dp")
    all_slots, width = param_part.shape
    cols, own_slots = width // shards, all_slots // owners
    low = param_part.astype(jnp.bfloat16)
    total = lax.dynamic_slice_in_dim(param_part, shard * cols, cols, axis=1)
    for j in range(1, shards):
        block = lax.dynamic_slice_in_dim(low, (shard ^ j) * cols, cols, axis=1)
        total = total + trade(block, "dp", j).astype(jnp.float32)
    low = total.astype(jnp.bfloat16)
    owned = total[:own_slots]
    for k in range(1, owners):
        block = low[k * own_slots : (k + 1) * own_slots]
        owned = owned + trade(block, "expert", k).astype(jnp.float32)
    return owned


def per_device(tokens, grad_out, slot_out, slot_params):
    owners, shards = lax.axis_size("expert"), lax.axis_size("dp")
    me = lax.axis_index("expert")
    all_params = gather_params(slot_params, owners, shards)
    slot_rows = fetch_outputs(slot_out, owners, me)
    logits = jnp.einsum("tbd,sd->tbs", tokens, all_params, preferred_element_type=jnp.float32)
    combine = jax.nn.softmax(logits, axis=-1)
    grad_slot = jnp.einsum(
        "tbs,tbd->bsd",
        combine.astype(jnp.bfloat16),
        grad_out,
        preferred_element_type=jnp.float32,
    ).astype(jnp.bfloat16)
    grad_slot_out = return_grads(grad_slot, owners, me)
    grad_comb = jnp.einsum("tbd,bsd->tbs", grad_out, slot_rows, preferred_element_type=jnp.float32)
    rowdot = jnp.sum(combine * grad_comb, axis=-1, keepdims=True)
    grad_logits = (combine * (grad_comb - rowdot)).astype(jnp.bfloat16)
    param_part = jnp.einsum("tbs,tbd->sd", grad_logits, tokens, preferred_element_type=jnp.float32)
    grad_params = reduce_params(param_part, owners, shards)
    grad_tok = jnp.einsum(
        "tbs,sd->tbd", grad_logits, all_params, preferred_element_type=jnp.float32
    ).astype(jnp.bfloat16)
    return (grad_tok, grad_slot_out, grad_params)


def solution(mesh):
    return jax.shard_map(
        per_device,
        mesh=mesh,
        in_specs=(
            P(None, ("dp", "expert"), None),
            P(None, ("dp", "expert"), None),
            P("expert", "dp", None),
            P("expert", None),
        ),
        out_specs=(P(None, ("dp", "expert"), None), P("expert", "dp", None), P("expert", "dp")),
        check_vma=False,
    )
```

```python
import jax
import jax.numpy as jnp
from jax import lax
from jax.experimental import pallas as pl
from jax.experimental.pallas import tpu as pltpu
from jax.sharding import PartitionSpec as P


UNITS = 4
OUT_UNITS = (2, 2)
BACK_UNITS = (3, 1)
LANES = 256


def partners(size, step):
    return [(i, i ^ step) for i in range(size)]


def trade(x, axis, step):
    return lax.ppermute(x, axis, partners(lax.axis_size(axis), step))


def gather_params(slot_params, owners, shards):
    shard = lax.axis_index("dp")
    _, width = slot_params.shape
    cols = width // shards
    mine = lax.dynamic_slice_in_dim(slot_params, shard * cols, cols, axis=1)
    blocks = [mine]
    for k in range(1, owners):
        blocks.append(trade(mine, "expert", k))
    part = jnp.concatenate(lax.optimization_barrier(blocks), axis=0)
    parts = [part]
    for j in range(1, shards):
        low = j & -j
        parts.append(trade(parts[j ^ low], "dp", low))
    parts = jnp.stack(lax.optimization_barrier(parts))
    return jnp.concatenate(
        [lax.dynamic_index_in_dim(parts, j ^ shard, 0, keepdims=False) for j in range(shards)],
        axis=1,
    )


def split_kernel(me_ref, x_ref, *refs):
    outs, stage = refs[:-1], refs[-1]
    turned = x_ref[...].astype(jnp.float32).transpose(1, 0, 2).astype(x_ref.dtype)
    stage[...] = turned.reshape(stage.shape)
    for k, out in enumerate(outs):
        out[...] = stage[me_ref[0] ^ k]


def split_slots(slot_out, me, owners, first, units):
    own_slots, img_all, width = slot_out.shape
    unit, images = own_slots // UNITS, img_all // owners
    block = pl.BlockSpec((images, unit, LANES), lambda u, j, me: (0, u, j))
    return pl.pallas_call(
        split_kernel,
        out_shape=[jax.ShapeDtypeStruct((images, units * unit, width), slot_out.dtype)] * owners,
        grid_spec=pltpu.PrefetchScalarGridSpec(
            num_scalar_prefetch=1,
            grid=(units, width // LANES),
            in_specs=[pl.BlockSpec((unit, img_all, LANES), lambda u, j, me: (first + u, 0, j))],
            out_specs=[block] * owners,
            scratch_shapes=[pltpu.VMEM((owners, images, unit, LANES), slot_out.dtype)],
        ),
    )(me[None], slot_out)


def join_kernel(me_ref, *refs):
    stage, out = refs[-1], refs[-2]
    owners, images, unit, lanes = stage.shape
    for k in range(owners):
        stage[me_ref[0] ^ k] = refs[k][...]
    rows = stage[...].reshape(owners * images, unit, lanes)
    out[...] = rows.astype(jnp.float32).transpose(1, 0, 2).astype(out.dtype)


def join_slots(blocks, whole, me, own_slots, first, units):
    owners = len(blocks)
    images, _, width = blocks[0].shape
    unit = own_slots // UNITS
    block = pl.BlockSpec((images, unit, LANES), lambda u, j, me: (0, u, j))
    in_specs, extra, aliases = [block] * owners, [], {}
    if whole is not None:
        in_specs, extra, aliases = in_specs + [pl.BlockSpec(memory_space=pl.ANY)], [whole], {owners + 1: 0}
    return pl.pallas_call(
        join_kernel,
        out_shape=jax.ShapeDtypeStruct((own_slots, owners * images, width), blocks[0].dtype),
        grid_spec=pltpu.PrefetchScalarGridSpec(
            num_scalar_prefetch=1,
            grid=(units, width // LANES),
            in_specs=in_specs,
            out_specs=pl.BlockSpec(
                (unit, owners * images, LANES), lambda u, j, me: (first + u, 0, j)
            ),
            scratch_shapes=[pltpu.VMEM((owners, images, unit, LANES), blocks[0].dtype)],
        ),
        input_output_aliases=aliases,
    )(me[None], *blocks, *extra)


def fetch_outputs(slot_out, owners, me):
    parts, first = [], 0
    for units in OUT_UNITS:
        blocks = split_slots(slot_out, me, owners, first, units)
        got = [blocks[0]]
        for k in range(1, owners):
            got.append(trade(blocks[k], "expert", k))
        parts.append(got)
        first += units
    parts = lax.optimization_barrier(parts)
    return jnp.concatenate([part[k] for k in range(owners) for part in parts], axis=1)


def return_grads(grad_slot, owners, me):
    _, all_slots, _ = grad_slot.shape
    own_slots = all_slots // owners
    unit = own_slots // UNITS
    out, first = None, 0
    for units in BACK_UNITS:
        blocks = []
        for k in range(owners):
            at = k * own_slots + first * unit
            block = grad_slot[:, at : at + units * unit]
            blocks.append(trade(block, "expert", k) if k else block)
        out = join_slots(blocks, out, me, own_slots, first, units)
        first += units
    return out


def reduce_params(param_part, owners, shards):
    shard = lax.axis_index("dp")
    all_slots, width = param_part.shape
    cols, own_slots = width // shards, all_slots // owners
    low = param_part.astype(jnp.bfloat16)
    total = lax.dynamic_slice_in_dim(param_part, shard * cols, cols, axis=1)
    for j in range(1, shards):
        block = lax.dynamic_slice_in_dim(low, (shard ^ j) * cols, cols, axis=1)
        block = trade(block, "dp", j)
        total = total + block.astype(jnp.float32)
    low = total.astype(jnp.bfloat16)
    owned = total[:own_slots]
    for k in range(1, owners):
        block = low[k * own_slots : (k + 1) * own_slots]
        owned = owned + trade(block, "expert", k).astype(jnp.float32)
    return owned


def per_device(tokens, grad_out, slot_out, slot_params):
    owners, shards = lax.axis_size("expert"), lax.axis_size("dp")
    me = lax.axis_index("expert")
    all_params = gather_params(slot_params, owners, shards)
    slot_rows = fetch_outputs(slot_out, owners, me)
    logits = jnp.einsum("tbd,sd->tbs", tokens, all_params, preferred_element_type=jnp.float32)
    combine = jax.nn.softmax(logits, axis=-1)
    grad_slot = jnp.einsum(
        "tbs,tbd->bsd",
        combine.astype(jnp.bfloat16),
        grad_out,
        preferred_element_type=jnp.float32,
    ).astype(jnp.bfloat16)
    grad_slot_out = return_grads(grad_slot, owners, me)
    grad_comb = jnp.einsum("tbd,bsd->tbs", grad_out, slot_rows, preferred_element_type=jnp.float32)
    rowdot = jnp.sum(combine * grad_comb, axis=-1, keepdims=True)
    grad_logits = (combine * (grad_comb - rowdot)).astype(jnp.bfloat16)
    param_part = jnp.einsum("tbs,tbd->sd", grad_logits, tokens, preferred_element_type=jnp.float32)
    grad_params = reduce_params(param_part, owners, shards)
    grad_tok = jnp.einsum(
        "tbs,sd->tbd", grad_logits, all_params, preferred_element_type=jnp.float32
    ).astype(jnp.bfloat16)
    return (grad_tok, grad_slot_out, grad_params)


def solution(mesh):
    return jax.shard_map(
        per_device,
        mesh=mesh,
        in_specs=(
            P(None, ("dp", "expert"), None),
            P(None, ("dp", "expert"), None),
            P("expert", "dp", None),
            P("expert", None),
        ),
        out_specs=(P(None, ("dp", "expert"), None), P("expert", "dp", None), P("expert", "dp")),
        check_vma=False,
    )
```
